32 devices in a mesh: cell: 16 (over z, y, core), tm: 2 (over x).
Axes of the slice: x: 2, y: 2, z: 4, core: 2. Of those that a mesh axis runs over, the one named last changes fastest.
Arguments:
- anomalies: float32 [32768, 2048], P('cell', 'tm'), may hold values from -6 to 6
- start_basis: float32 [2048, 128], P('tm'), may hold values from -0.125 to 0.125
Outputs:
- patterns: float32 [32768, 128], P(('cell', 'tm'))
The draws below stay inside these ranges and needn't reach their ends.
All inputs are finite; a program needn't handle non-finite values.
Results may differ from the reference program's by a relative error of at most 0.0003.
Values sent between devices are 32-bit elements; how exact they have to be, the bound alone decides.
A program may use at most 64 MiB of HBM per device.

```python
import jax
import jax.numpy as jnp
from jax import lax

K = 128
ITERS = 2
CELLS = 32768
HOURS = 2048


def block_scale(stream_key, shape, split, low, high):
    def one(position, blocks):
        steps = jax.random.uniform(jax.random.fold_in(jax.random.fold_in(stream_key, 6), position), (blocks,), jnp.float32, low / len(split), high / len(split))
        return jnp.repeat(jnp.exp(steps), shape[position] // blocks).reshape((-1,) + (1,) * (len(shape) - position - 1))

    loudness = one(*split[0])
    for cut in split[1:]:
        loudness = loudness * one(*cut)
    return loudness


def gaussian(rng, extent, spread, limit, cuts=(), held_as=jnp.bfloat16):
    drawn = jax.random.normal(rng, extent, jnp.float32) * spread
    if len(cuts) > 0:
        drawn = block_scale(rng, extent, cuts, -0.22, 0.18) * drawn
    return jnp.clip(drawn, min=-limit, max=limit).astype(held_as)


def setup_inputs(seed: int = 0) -> dict:
    key_list = jax.random.split(jax.random.key(seed), 3)
    anomalies = gaussian(key_list[0], (CELLS, HOURS), 1.0, 6.0, ((0, 16), (1, 2)), jnp.float32)
    start_basis = gaussian(key_list[1], (HOURS, K), HOURS ** -0.5, 0.125, ((0, 2),), jnp.float32)
    return dict(anomalies=anomalies, start_basis=start_basis)


def reference(anomalies, start_basis):
    full = lax.Precision.HIGHEST
    basis = start_basis
    for step in range(ITERS):
        spatial = jnp.dot(anomalies.astype(jnp.float32), basis.astype(jnp.float32), precision=full, preferred_element_type=jnp.float32)
        image = lax.dot_general(anomalies.astype(jnp.float32), spatial.astype(jnp.float32), (((0,), (0,)), ((), ())), precision=full, preferred_element_type=jnp.float32)
        gram = lax.dot_general(image.astype(jnp.float32), image.astype(jnp.float32), (((0,), (0,)), ((), ())), precision=full, preferred_element_type=jnp.float32)
        lower = jnp.linalg.cholesky(gram)
        basis = jax.scipy.linalg.solve_triangular(lower, image.T, lower=True).T
    return jnp.dot(anomalies.astype(jnp.float32), basis.astype(jnp.float32), precision=full, preferred_element_type=jnp.float32)
```

```python
import functools

import jax
import jax.numpy as jnp
from jax import lax
from jax.experimental import pallas as pl
from jax.experimental.pallas import tpu as pltpu
from jax.sharding import PartitionSpec as P

ITERS = 2
GROUPS = 2
CHUNKS = 4
PAIR = 2
SUB = 8
MESH = pl.DeviceIdType.MESH
NT = (((1,), (1,)), ((), ()))
NN = (((1,), (0,)), ((), ()))


def split(x):
    hi = x.astype(jnp.bfloat16)
    return hi, (x - hi.astype(jnp.float32)).astype(jnp.bfloat16)


def dot3(x, hi, lo, dims):
    rows = x.shape[0]
    x_hi, x_lo = split(x)
    both = lax.dot_general(
        jnp.concatenate([x_hi, x_lo], axis=0), hi, dims, preferred_element_type=jnp.float32
    )
    low = lax.dot_general(x_hi, lo, dims, preferred_element_type=jnp.float32)
    return both[:rows] + (both[rows:] + low)


def dot_full(x, y, dims):
    return lax.dot_general(
        x, y, dims, precision=lax.Precision.HIGHEST, preferred_element_type=jnp.float32
    )


def eliminate(mat, first, last):
    k = mat.shape[1]
    row = lax.broadcasted_iota(jnp.int32, (k, 1), 0)

    def body(step, carry):
        left, right = carry
        live = k - step * SUB
        for j in range(SUB):
            col = jnp.broadcast_to(left[:, j : j + 1], (k, k))
            inv = 1.0 / col[j : j + 1, :]
            factor = jnp.where((row > j) & (row < live), col, 0.0)
            l_row = left[j : j + 1, :] * inv
            r_row = right[j : j + 1, :] * inv
            left = left - factor * l_row
            right = right - factor * r_row
        diag = jnp.sum(
            jnp.where(
                lax.broadcasted_iota(jnp.int32, (SUB, k), 0)
                == lax.broadcasted_iota(jnp.int32, (SUB, k), 1),
                left[:SUB],
                0.0,
            ),
            axis=1,
            keepdims=True,
        )
        done = right[:SUB] * lax.rsqrt(diag)
        right = jnp.concatenate([right[SUB:], done], axis=0)
        left = jnp.concatenate([left[SUB:], left[:SUB]], axis=0)
        left = pltpu.roll(left, k - SUB, 1)
        return left, right

    left, right = lax.fori_loop(first, last, body, (mat[0], mat[1]))
    mat[0] = left
    mat[1] = right


def kernel(
    n_cell, n_tm, a_hbm, b_ref, out_ref,
    a_f32, a_hi, a_lo, send_s, recv_s, send_i, recv_a, half, recv_b, full, norm,
    gram_s, gram_r, mat1, mat2, send_p, recv_p, own_p,
    load_sem, s_ss, s_rs, a_ss, a_rs, b_ss, b_rs, c_ss, c_rs, d_ss, d_rs,
    g_ss, g_rs, p_ss, p_rs,
):
    cell, tm = lax.axis_index("cell"), lax.axis_index("tm")
    chip, core = cell // PAIR, cell % PAIR
    n_chip = n_cell // PAIR
    cells, hours = a_hbm.shape
    k = b_ref.shape[1]
    kg = k // GROUPS
    rows = cells // CHUNKS
    mid = hours // PAIR
    piece_rows = max(SUB, kg // n_chip)
    n_down = kg // piece_rows
    piece_cols = mid // (n_chip // n_down)
    part = cells // n_tm

    loads = []
    for c in range(CHUNKS):
        block = pl.ds(c * rows, rows)
        copy = pltpu.make_async_copy(a_hbm.at[block], a_f32.at[block], load_sem.at[c])
        copy.start()
        loads.append(copy)

    def tm_peer(d):
        return {"cell": cell, "tm": (tm + d) % n_tm}

    def chip_peer(d):
        return {"cell": ((chip + d) % n_chip) * PAIR + core, "tm": tm}

    sibling = {"cell": chip * PAIR + (1 - core), "tm": tm}
    peers = [tm_peer(d) for d in range(1, n_tm)]
    peers += [chip_peer(d) for d in range(1, n_chip)] + [sibling]
    barrier = pltpu.get_barrier_semaphore()
    for peer in peers:
        pl.semaphore_signal(barrier, inc=1, device_id=peer, device_id_type=MESH)
    pl.semaphore_wait(barrier, len(peers))

    started = {}

    def send(key, src, dst, ss, rs, peer):
        copy = pltpu.make_async_remote_copy(
            src_ref=src, dst_ref=dst, send_sem=ss, recv_sem=rs,
            device_id=peer, device_id_type=MESH,
        )
        copy.start()
        started[key] = copy

    def arrived(*key):
        started[key].wait_recv()

    def send_spatial(it, g, c):
        for d in range(1, n_tm):
            send(("s", it, g, c, d), send_s.at[it, g, c], recv_s.at[it, g, c, d - 1],
                 s_ss.at[it, g, c, d - 1], s_rs.at[it, g, c, d - 1], tm_peer(d))

    def chunk(it, g, c):
        for d in range(1, n_tm):
            arrived("s", it, g, c, d)
        spatial = send_s[it, g, c]
        for d in range(1, n_tm):
            spatial = spatial + recv_s[it, g, c, d - 1]
        block = pl.ds(c * rows, rows)
        term = dot3(spatial, a_hi[block, :], a_lo[block, :], NN)
        send_i[it, g] = term if c == 0 else send_i[it, g] + term

    mine = pl.ds(pl.multiple_of(core * mid, mid), mid)
    other = pl.ds(pl.multiple_of((1 - core) * mid, mid), mid)

    def place(q):
        down = pl.ds(pl.multiple_of((q % n_down) * piece_rows, piece_rows), piece_rows)
        return down, (q // n_down) * piece_cols

    def sum_pair(it, g):
        send(("a", it, g), send_i.at[it, g, :, other], recv_a.at[it, g],
             a_ss.at[it, g], a_rs.at[it, g], sibling)

    def sum_chips(it, g):
        arrived("a", it, g)
        half[it, g] = send_i[it, g, :, mine] + recv_a[it, g]
        for d in range(1, n_chip):
            down, across = place((chip + d) % n_chip)
            across = pl.ds(pl.multiple_of(across, piece_cols), piece_cols)
            send(("b", it, g, d), half.at[it, g, down, across], recv_b.at[it, g, d - 1],
                 b_ss.at[it, g, d - 1], b_rs.at[it, g, d - 1], chip_peer(d))

    def give_chips(it, g):
        down, across = place(chip)
        at_half = pl.ds(pl.multiple_of(across, piece_cols), piece_cols)
        at_full = pl.ds(pl.multiple_of(core * mid + across, piece_cols), piece_cols)
        total = half[it, g, down, at_half]
        for d in range(1, n_chip):
            arrived("b", it, g, d)
            total = total + recv_b[it, g, d - 1]
        full[it, g, down, at_full] = total
        for d in range(1, n_chip):
            spot = full.at[it, g, down, at_full]
            send(("c", it, g, d), spot, spot,
                 c_ss.at[it, g, d - 1], c_rs.at[it, g, d - 1], chip_peer(d))

    def give_pair(it, g):
        for d in range(1, n_chip):
            down, across = place((chip + n_chip - d) % n_chip)
            at_full = pl.ds(pl.multiple_of(core * mid + across, piece_cols), piece_cols)
            spot = full.at[it, g, down, at_full]
            pltpu.make_async_remote_copy(
                src_ref=spot, dst_ref=spot, send_sem=c_ss.at[it, g, d - 1],
                recv_sem=c_rs.at[it, g, d - 1], device_id=chip_peer(d), device_id_type=MESH,
            ).wait_recv()
        spot = full.at[it, g, :, mine]
        send(("d", it, g), spot, spot, d_ss.at[it, g], d_rs.at[it, g], sibling)

    def complete(it, g):
        spot = full.at[it, g, :, other]
        pltpu.make_async_remote_copy(
            src_ref=spot, dst_ref=spot, send_sem=d_ss.at[it, g], recv_sem=d_rs.at[it, g],
            device_id=sibling, device_id_type=MESH,
        ).wait_recv()

    def next_spatial(it, g):
        image = full[it - 1, g]
        for c in range(CHUNKS):
            block = pl.ds(c * rows, rows)
            send_s[it, g, c] = dot3(image, a_hi[block, :], a_lo[block, :], NT)
            send_spatial(it, g, c)

    def send_gram(it, blocks):
        image = jnp.concatenate(blocks, axis=0)
        gram_s[it] = dot_full(image, image, NT)
        for d in range(1, n_tm):
            send(("g", it, d), gram_s.at[it], gram_r.at[it, d - 1],
                 g_ss.at[it, d - 1], g_rs.at[it, d - 1], tm_peer(d))

    def take_gram(it, mat):
        gram = gram_s[it]
        for d in range(1, n_tm):
            arrived("g", it, d)
            gram = gram + gram_r[it, d - 1]
        mat[0] = gram
        mat[1] = (
            lax.broadcasted_iota(jnp.int32, (k, k), 0)
            == lax.broadcasted_iota(jnp.int32, (k, k), 1)
        ).astype(jnp.float32)

    def normalise(g):
        raw = jnp.concatenate([full[1, h] for h in range(g + 1)], axis=0)
        norm[g] = dot_full(mat1[1, g * kg : (g + 1) * kg, : (g + 1) * kg], raw, NN)

    def cells_of(owner):
        return pl.ds(pl.multiple_of(owner * part, part), part)

    def send_patterns(g):
        for d in range(1, n_tm):
            block = cells_of((tm + d) % n_tm)
            send_p[g, d - 1] = dot3(norm[g], a_hi[block, :], a_lo[block, :], NT)
            send(("p", g, d), send_p.at[g, d - 1], recv_p.at[g, d - 1],
                 p_ss.at[g, d - 1], p_rs.at[g, d - 1], tm_peer(d))

    def own_patterns(g):
        block = cells_of(tm)
        own_p[g] = dot3(norm[g], a_hi[block, :], a_lo[block, :], NT)

    steps = k // SUB

    def part_of(n):
        eliminate(mat1, n * steps // 4, (n + 1) * steps // 4)

    basis = b_ref[...].T
    for c in range(CHUNKS):
        loads[c].wait()
        block = pl.ds(c * rows, rows)
        hi, lo = split(a_f32[block, :])
        a_hi[block, :] = hi
        a_lo[block, :] = lo
        spatial = dot3(basis, hi, lo, NT)
        for g in range(GROUPS):
            send_s[0, g, c] = spatial[g * kg : (g + 1) * kg]
        send_spatial(0, 0, c)
    for c in range(CHUNKS):
        send_spatial(0, 1, c)

    for c in range(CHUNKS):
        chunk(0, 0, c)
    sum_pair(0, 0)
    chunk(0, 1, 0)
    sum_chips(0, 0)
    chunk(0, 1, 1)
    chunk(0, 1, 2)
    give_chips(0, 0)
    chunk(0, 1, 3)
    sum_pair(0, 1)
    give_pair(0, 0)
    sum_chips(0, 1)
    complete(0, 0)
    next_spatial(1, 0)
    give_chips(0, 1)
    chunk(1, 0, 0)
    chunk(1, 0, 1)
    give_pair(0, 1)
    chunk(1, 0, 2)
    complete(0, 1)
    send_gram(0, [full[0, g] for g in range(GROUPS)])
    next_spatial(1, 1)
    chunk(1, 0, 3)
    sum_pair(1, 0)
    take_gram(0, mat1)
    sum_chips(1, 0)
    part_of(0)
    chunk(1, 1, 0)
    part_of(1)
    chunk(1, 1, 1)
    give_chips(1, 0)
    part_of(2)
    chunk(1, 1, 2)
    give_pair(1, 0)
    part_of(3)
    chunk(1, 1, 3)
    sum_pair(1, 1)
    complete(1, 0)
    normalise(0)
    sum_chips(1, 1)
    send_patterns(0)
    own_patterns(0)
    give_chips(1, 1)
    give_pair(1, 1)
    complete(1, 1)
    normalise(1)
    send_gram(1, [norm[g] for g in range(GROUPS)])
    send_patterns(1)
    take_gram(1, mat2)
    eliminate(mat2, 0, steps)
    own_patterns(1)
    blocks = []
    for g in range(GROUPS):
        total = own_p[g]
        for d in range(1, n_tm):
            arrived("p", g, d)
            total = total + recv_p[g, d - 1]
        blocks.append(total)
    out_ref[...] = dot_full(mat2[1], jnp.concatenate(blocks, axis=0), NN).T
    for copy in started.values():
        copy.wait_send()


def on_device(n_cell, n_tm, anomalies, start_basis):
    cells, hours = anomalies.shape
    k = start_basis.shape[1]
    kg, rows, mid = k // GROUPS, cells // CHUNKS, hours // PAIR
    n_chip = n_cell // PAIR
    piece_rows = max(SUB, kg // n_chip)
    piece_cols = mid // (n_chip // (kg // piece_rows))
    part = cells // n_tm
    far, near = n_tm - 1, n_chip - 1
    f32, bf16 = jnp.float32, jnp.bfloat16
    dma = pltpu.SemaphoreType.DMA
    pair_sem = lambda *shape: [dma(shape), dma(shape)]
    return pl.pallas_call(
        functools.partial(kernel, n_cell, n_tm),
        out_shape=jax.ShapeDtypeStruct((part, k), f32),
        in_specs=[
            pl.BlockSpec(memory_space=pl.ANY),
            pl.BlockSpec(memory_space=pltpu.VMEM),
        ],
        out_specs=pl.BlockSpec(memory_space=pltpu.VMEM),
        scratch_shapes=[
            pltpu.VMEM((cells, hours), f32),
            pltpu.VMEM((cells, hours), bf16),
            pltpu.VMEM((cells, hours), bf16),
            pltpu.VMEM((ITERS, GROUPS, CHUNKS, kg, rows), f32),
            pltpu.VMEM((ITERS, GROUPS, CHUNKS, far, kg, rows), f32),
            pltpu.VMEM((ITERS, GROUPS, kg, hours), f32),
            pltpu.VMEM((ITERS, GROUPS, kg, mid), f32),
            pltpu.VMEM((ITERS, GROUPS, kg, mid), f32),
            pltpu.VMEM((ITERS, GROUPS, near, piece_rows, piece_cols), f32),
            pltpu.VMEM((ITERS, GROUPS, kg, hours), f32),
            pltpu.VMEM((GROUPS, kg, hours), f32),
            pltpu.VMEM((ITERS, k, k), f32),
            pltpu.VMEM((ITERS, far, k, k), f32),
            pltpu.VMEM((2, k, k), f32),
            pltpu.VMEM((2, k, k), f32),
            pltpu.VMEM((GROUPS, far, kg, part), f32),
            pltpu.VMEM((GROUPS, far, kg, part), f32),
            pltpu.VMEM((GROUPS, kg, part), f32),
            dma((CHUNKS,)),
            *pair_sem(ITERS, GROUPS, CHUNKS, far),
            *pair_sem(ITERS, GROUPS),
            *pair_sem(ITERS, GROUPS, near),
            *pair_sem(ITERS, GROUPS, near),
            *pair_sem(ITERS, GROUPS),
            *pair_sem(ITERS, far),
            *pair_sem(GROUPS, far),
        ],
        compiler_params=pltpu.CompilerParams(
            collective_id=0, has_side_effects=True, vmem_limit_bytes=60 * 1024 * 1024
        ),
    )(anomalies, start_basis)


def solution(mesh):
    in_specs = (P("cell", "tm"), P("tm", None))
    out_specs = P(("cell", "tm"), None)
    return jax.shard_map(
        functools.partial(on_device, mesh.shape["cell"], mesh.shape["tm"]),
        mesh=mesh, in_specs=in_specs, out_specs=out_specs, check_vma=False,
    )
```

```python
import functools

import jax
import jax.numpy as jnp
from jax import lax
from jax.experimental import pallas as pl
from jax.experimental.pallas import tpu as pltpu
from jax.sharding import PartitionSpec as P

ITERS = 2
GROUPS = 2
CHUNKS = 4
PAIR = 2
SUB = 8
MESH = pl.DeviceIdType.MESH
NT = (((1,), (1,)), ((), ()))
NN = (((1,), (0,)), ((), ()))


def split(x):
    hi = x.astype(jnp.bfloat16)
    return hi, (x - hi.astype(jnp.float32)).astype(jnp.bfloat16)


def dot3(x, hi, lo, dims):
    rows = x.shape[0]
    x_hi, x_lo = split(x)
    both = lax.dot_general(
        jnp.concatenate([x_hi, x_lo], axis=0), hi, dims, preferred_element_type=jnp.float32
    )
    low = lax.dot_general(x_hi, lo, dims, preferred_element_type=jnp.float32)
    return both[:rows] + (both[rows:] + low)


def dot_full(x, y, dims):
    return lax.dot_general(
        x, y, dims, precision=lax.Precision.HIGHEST, preferred_element_type=jnp.float32
    )


def inverse_factor(gram):
    k = gram.shape[0]
    row = lax.broadcasted_iota(jnp.int32, (k, 1), 0)
    square = (k, k)
    eye = lax.broadcasted_iota(jnp.int32, square, 0) == lax.broadcasted_iota(jnp.int32, square, 1)
    corner = (SUB, 2 * k)
    diagonal = lax.broadcasted_iota(jnp.int32, corner, 0) == lax.broadcasted_iota(
        jnp.int32, corner, 1
    )

    def body(step, both):
        live = k - step * SUB
        for j in range(SUB):
            col = jnp.broadcast_to(both[:, j : j + 1], (k, 2 * k))
            scaled = both[j : j + 1, :] * (1.0 / col[j : j + 1, :])
            both = both - jnp.where((row > j) & (row < live), col, 0.0) * scaled
        pivots = jnp.sum(jnp.where(diagonal, both[:SUB], 0.0), axis=1, keepdims=True)
        done = both[:SUB] * lax.rsqrt(pivots)
        return pltpu.roll(jnp.concatenate([both[SUB:], done], axis=0), 2 * k - SUB, 1)

    start = jnp.concatenate([gram, eye.astype(jnp.float32)], axis=1)
    return lax.fori_loop(0, k // SUB, body, start)[:, :k]


def kernel(
    n_cell, n_tm, a_hbm, b_ref, out_ref,
    a_f32, a_hi, a_lo, send_s, recv_s, send_i, recv_a, half, recv_b, full, norm,
    gram_s, gram_r, lin, send_p, recv_p, own_p,
    load_sem, s_ss, s_rs, a_ss, a_rs, b_ss, b_rs, c_ss, c_rs, d_ss, d_rs,
    g_ss, g_rs, p_ss, p_rs,
):
    cell, tm = lax.axis_index("cell"), lax.axis_index("tm")
    chip, core = cell // PAIR, cell % PAIR
    n_chip = n_cell // PAIR
    cells, hours = a_hbm.shape
    k = b_ref.shape[1]
    kg = k // GROUPS
    rows = cells // CHUNKS
    mid = hours // PAIR
    piece_rows = max(SUB, kg // n_chip)
    n_down = kg // piece_rows
    piece_cols = mid // (n_chip // n_down)
    part = cells // n_tm

    loads = []
    for c in range(CHUNKS):
        block = pl.ds(c * rows, rows)
        copy = pltpu.make_async_copy(a_hbm.at[block], a_f32.at[block], load_sem.at[c])
        copy.start()
        loads.append(copy)

    def tm_peer(d):
        return {"cell": cell, "tm": (tm + d) % n_tm}

    def chip_peer(d):
        return {"cell": ((chip + d) % n_chip) * PAIR + core, "tm": tm}

    sibling = {"cell": chip * PAIR + (1 - core), "tm": tm}
    peers = [tm_peer(d) for d in range(1, n_tm)]
    peers += [chip_peer(d) for d in range(1, n_chip)] + [sibling]
    barrier = pltpu.get_barrier_semaphore()
    for peer in peers:
        pl.semaphore_signal(barrier, inc=1, device_id=peer, device_id_type=MESH)
    pl.semaphore_wait(barrier, len(peers))

    started = {}

    def send(key, src, dst, ss, rs, peer):
        copy = pltpu.make_async_remote_copy(
            src_ref=src, dst_ref=dst, send_sem=ss, recv_sem=rs,
            device_id=peer, device_id_type=MESH,
        )
        copy.start()
        started[key] = copy

    def arrived(*key):
        started[key].wait_recv()

    def send_spatial(it, g, c):
        for d in range(1, n_tm):
            send(("s", it, g, c, d), send_s.at[it, g, c], recv_s.at[it, g, c, d - 1],
                 s_ss.at[it, g, c, d - 1], s_rs.at[it, g, c, d - 1], tm_peer(d))

    def chunk(it, g, c):
        for d in range(1, n_tm):
            arrived("s", it, g, c, d)
        spatial = send_s[it, g, c]
        for d in range(1, n_tm):
            spatial = spatial + recv_s[it, g, c, d - 1]
        block = pl.ds(c * rows, rows)
        term = dot3(spatial, a_hi[block, :], a_lo[block, :], NN)
        send_i[it, g] = term if c == 0 else send_i[it, g] + term

    mine = pl.ds(pl.multiple_of(core * mid, mid), mid)
    other = pl.ds(pl.multiple_of((1 - core) * mid, mid), mid)

    def place(q):
        down = pl.ds(pl.multiple_of((q % n_down) * piece_rows, piece_rows), piece_rows)
        return down, (q // n_down) * piece_cols

    def sum_pair(it, g):
        send(("a", it, g), send_i.at[it, g, :, other], recv_a.at[it, g],
             a_ss.at[it, g], a_rs.at[it, g], sibling)

    def sum_chips(it, g):
        arrived("a", it, g)
        half[it, g] = send_i[it, g, :, mine] + recv_a[it, g]
        for d in range(1, n_chip):
            down, across = place((chip + d) % n_chip)
            across = pl.ds(pl.multiple_of(across, piece_cols), piece_cols)
            send(("b", it, g, d), half.at[it, g, down, across], recv_b.at[it, g, d - 1],
                 b_ss.at[it, g, d - 1], b_rs.at[it, g, d - 1], chip_peer(d))

    def give_chips(it, g):
        down, across = place(chip)
        at_half = pl.ds(pl.multiple_of(across, piece_cols), piece_cols)
        at_full = pl.ds(pl.multiple_of(core * mid + across, piece_cols), piece_cols)
        total = half[it, g, down, at_half]
        for d in range(1, n_chip):
            arrived("b", it, g, d)
            total = total + recv_b[it, g, d - 1]
        full[it, g, down, at_full] = total
        for d in range(1, n_chip):
            spot = full.at[it, g, down, at_full]
            send(("c", it, g, d), spot, spot,
                 c_ss.at[it, g, d - 1], c_rs.at[it, g, d - 1], chip_peer(d))

    def give_pair(it, g):
        for d in range(1, n_chip):
            down, across = place((chip + n_chip - d) % n_chip)
            at_full = pl.ds(pl.multiple_of(core * mid + across, piece_cols), piece_cols)
            spot = full.at[it, g, down, at_full]
            pltpu.make_async_remote_copy(
                src_ref=spot, dst_ref=spot, send_sem=c_ss.at[it, g, d - 1],
                recv_sem=c_rs.at[it, g, d - 1], device_id=chip_peer(d), device_id_type=MESH,
            ).wait_recv()
        spot = full.at[it, g, :, mine]
        send(("d", it, g), spot, spot, d_ss.at[it, g], d_rs.at[it, g], sibling)

    def complete(it, g):
        spot = full.at[it, g, :, other]
        pltpu.make_async_remote_copy(
            src_ref=spot, dst_ref=spot, send_sem=d_ss.at[it, g], recv_sem=d_rs.at[it, g],
            device_id=sibling, device_id_type=MESH,
        ).wait_recv()

    def next_spatial(it, g):
        image = full[it - 1, g]
        for c in range(CHUNKS):
            block = pl.ds(c * rows, rows)
            send_s[it, g, c] = dot3(image, a_hi[block, :], a_lo[block, :], NT)
            send_spatial(it, g, c)

    def send_gram(it, g, blocks):
        gram_s[it, g] = dot_full(blocks[g], jnp.concatenate(blocks, axis=0), NT)
        for d in range(1, n_tm):
            send(("g", it, g, d), gram_s.at[it, g], gram_r.at[it, g, d - 1],
                 g_ss.at[it, g, d - 1], g_rs.at[it, g, d - 1], tm_peer(d))

    def factor(it, g):
        gram = gram_s[it, g]
        for d in range(1, n_tm):
            arrived("g", it, g, d)
            gram = gram + gram_r[it, g, d - 1]
        if g == 0:
            inv = inverse_factor(gram[:, :kg])
            lin[it, 0] = jnp.concatenate([inv, jnp.zeros_like(inv)], axis=1)
        else:
            first = lin[it, 0, :, :kg]
            below = dot_full(gram[:, :kg], first, NT)
            inv = inverse_factor(gram[:, kg:] - dot_full(below, below, NT))
            left = dot_full(dot_full(inv, below, NN), first, NN)
            lin[it, 1] = jnp.concatenate([-left, inv], axis=1)

    def normalise(g):
        raw = jnp.concatenate([full[1, h] for h in range(g + 1)], axis=0)
        norm[g] = dot_full(lin[0, g, :, : (g + 1) * kg], raw, NN)

    def cells_of(owner):
        return pl.ds(pl.multiple_of(owner * part, part), part)

    def send_patterns(g):
        for d in range(1, n_tm):
            block = cells_of((tm + d) % n_tm)
            send_p[g, d - 1] = dot3(norm[g], a_hi[block, :], a_lo[block, :], NT)
            send(("p", g, d), send_p.at[g, d - 1], recv_p.at[g, d - 1],
                 p_ss.at[g, d - 1], p_rs.at[g, d - 1], tm_peer(d))

    def own_patterns(g):
        block = cells_of(tm)
        own_p[g] = dot3(norm[g], a_hi[block, :], a_lo[block, :], NT)

    basis = b_ref[...].T
    for c in range(CHUNKS):
        loads[c].wait()
        block = pl.ds(c * rows, rows)
        hi, lo = split(a_f32[block, :])
        a_hi[block, :] = hi
        a_lo[block, :] = lo
        spatial = dot3(basis, hi, lo, NT)
        for g in range(GROUPS):
            send_s[0, g, c] = spatial[g * kg : (g + 1) * kg]
        send_spatial(0, 0, c)
    for c in range(CHUNKS):
        send_spatial(0, 1, c)

    for c in range(CHUNKS):
        chunk(0, 0, c)
    sum_pair(0, 0)
    sum_chips(0, 0)
    chunk(0, 1, 0)
    chunk(0, 1, 1)
    give_chips(0, 0)
    chunk(0, 1, 2)
    chunk(0, 1, 3)
    sum_pair(0, 1)
    give_pair(0, 0)
    sum_chips(0, 1)
    complete(0, 0)
    next_spatial(1, 0)
    give_chips(0, 1)
    send_gram(0, 0, [full[0, 0], full[0, 0]])
    give_pair(0, 1)
    chunk(1, 0, 0)
    complete(0, 1)
    next_spatial(1, 1)
    chunk(1, 0, 1)
    send_gram(0, 1, [full[0, 0], full[0, 1]])
    chunk(1, 0, 2)
    chunk(1, 0, 3)
    sum_pair(1, 0)
    sum_chips(1, 0)
    factor(0, 0)
    chunk(1, 1, 0)
    chunk(1, 1, 1)
    chunk(1, 1, 2)
    give_chips(1, 0)
    chunk(1, 1, 3)
    sum_pair(1, 1)
    give_pair(1, 0)
    sum_chips(1, 1)
    complete(1, 0)
    normalise(0)
    send_patterns(0)
    send_gram(1, 0, [norm[0], norm[0]])
    factor(0, 1)
    give_chips(1, 1)
    factor(1, 0)
    give_pair(1, 1)
    own_patterns(0)
    complete(1, 1)
    normalise(1)
    send_gram(1, 1, [norm[0], norm[1]])
    send_patterns(1)
    factor(1, 1)
    own_patterns(1)
    blocks = []
    for g in range(GROUPS):
        total = own_p[g]
        for d in range(1, n_tm):
            arrived("p", g, d)
            total = total + recv_p[g, d - 1]
        blocks.append(total)
    out_ref[...] = dot_full(
        jnp.concatenate([lin[1, g] for g in range(GROUPS)], axis=0),
        jnp.concatenate(blocks, axis=0), NN,
    ).T
    for copy in started.values():
        copy.wait_send()


def on_device(n_cell, n_tm, anomalies, start_basis):
    cells, hours = anomalies.shape
    k = start_basis.shape[1]
    kg, rows, mid = k // GROUPS, cells // CHUNKS, hours // PAIR
    n_chip = n_cell // PAIR
    piece_rows = max(SUB, kg // n_chip)
    piece_cols = mid // (n_chip // (kg // piece_rows))
    part = cells // n_tm
    far, near = n_tm - 1, n_chip - 1
    f32, bf16 = jnp.float32, jnp.bfloat16
    dma = pltpu.SemaphoreType.DMA
    pair_sem = lambda *shape: [dma(shape), dma(shape)]
    return pl.pallas_call(
        functools.partial(kernel, n_cell, n_tm),
        out_shape=jax.ShapeDtypeStruct((part, k), f32),
        in_specs=[
            pl.BlockSpec(memory_space=pl.ANY),
            pl.BlockSpec(memory_space=pltpu.VMEM),
        ],
        out_specs=pl.BlockSpec(memory_space=pltpu.VMEM),
        scratch_shapes=[
            pltpu.VMEM((cells, hours), f32),
            pltpu.VMEM((cells, hours), bf16),
            pltpu.VMEM((cells, hours), bf16),
            pltpu.VMEM((ITERS, GROUPS, CHUNKS, kg, rows), f32),
            pltpu.VMEM((ITERS, GROUPS, CHUNKS, far, kg, rows), f32),
            pltpu.VMEM((ITERS, GROUPS, kg, hours), f32),
            pltpu.VMEM((ITERS, GROUPS, kg, mid), f32),
            pltpu.VMEM((ITERS, GROUPS, kg, mid), f32),
            pltpu.VMEM((ITERS, GROUPS, near, piece_rows, piece_cols), f32),
            pltpu.VMEM((ITERS, GROUPS, kg, hours), f32),
            pltpu.VMEM((GROUPS, kg, hours), f32),
            pltpu.VMEM((ITERS, GROUPS, kg, k), f32),
            pltpu.VMEM((ITERS, GROUPS, far, kg, k), f32),
            pltpu.VMEM((ITERS, GROUPS, kg, k), f32),
            pltpu.VMEM((GROUPS, far, kg, part), f32),
            pltpu.VMEM((GROUPS, far, kg, part), f32),
            pltpu.VMEM((GROUPS, kg, part), f32),
            dma((CHUNKS,)),
            *pair_sem(ITERS, GROUPS, CHUNKS, far),
            *pair_sem(ITERS, GROUPS),
            *pair_sem(ITERS, GROUPS, near),
            *pair_sem(ITERS, GROUPS, near),
            *pair_sem(ITERS, GROUPS),
            *pair_sem(ITERS, GROUPS, far),
            *pair_sem(GROUPS, far),
        ],
        compiler_params=pltpu.CompilerParams(
            collective_id=0, has_side_effects=True, vmem_limit_bytes=60 * 1024 * 1024
        ),
    )(anomalies, start_basis)


def solution(mesh):
    in_specs = (P("cell", "tm"), P("tm", None))
    out_specs = P(("cell", "tm"), None)
    return jax.shard_map(
        functools.partial(on_device, mesh.shape["cell"], mesh.shape["tm"]),
        mesh=mesh, in_specs=in_specs, out_specs=out_specs, check_vma=False,
    )
```
